32 devices in a mesh: dp: 8 (over z, x), seq: 4 (over y, core).
Axes of the slice: x: 2, y: 2, z: 4, core: 2. Of those that a mesh axis runs over, the one named last changes fastest.
Arguments:
- tokens: bfloat16 [4608, 3584], P('dp'), may hold values from -6 to 6
- positions: int32 [3, 4608], P(None, 'dp'), may hold values from 0 to 2047
- loss_mask: int32 [4608], P('dp'), may hold values from 0 to 1, as said below
- sample_tokens: int32 [8, 3], replicated, may hold values from 96 to 384, as said below
- dest_slot: int32 [4608], P('dp'), may hold values from 0 to 6143, as said below
- norm_gain: float32 [3584], replicated, may hold values from 0.5 to 1.5
- q_weight: bfloat16 [3584, 2048], P(None, 'seq'), may hold values from -0.09375 to 0.09375
- k_weight: bfloat16 [3584, 512], P(None, 'seq'), may hold values from -0.09375 to 0.09375
- v_weight: bfloat16 [3584, 512], P(None, 'seq'), may hold values from -0.09375 to 0.09375
- q_bias: float32 [2048], P('seq'), may hold values from -3 to 3
- k_bias: float32 [512], P('seq'), may hold values from -3 to 3
- v_bias: float32 [512], P('seq'), may hold values from -3 to 3
- o_weight: bfloat16 [2048, 3584], P('seq'), may hold values from -0.125 to 0.125
Outputs:
- mixed: bfloat16 [6144, 3584], P(('dp', 'seq'))
- token_weight: float32 [6144], P(('dp', 'seq'))
The draws below stay inside these ranges and needn't reach their ends.
Inputs may be any that keep to these rules, and one draw needn't show every extreme that they name: `sample_tokens`: row r gives the token counts of the samples in the buckets of receiver r, of 384, 192 and 192 slots; each count lies between half of its bucket's slots and all of them. Some receiver has all three buckets full. All counts together equal the number of rows of tokens. `dest_slot`: every row has a slot of its own, and the slots that rows take are exactly the first sample_tokens[r, b] slots of each bucket b of each receiver r. Of the rows of one sender at most 96 go to one receiver; a receiver whose buckets are all full takes exactly 96 rows from every sender. `loss_mask`: the first of each sender's 576 rows is 1.
All inputs are finite; a program needn't handle non-finite values.
Results may differ from the reference program's by a relative error of at most 0.015.
Values may be sent and summed in bfloat16 or wider, within the bound.
A program may use at most 128 MiB of HBM per device.

```python
import math
import jax
import jax.numpy as jnp
from jax import lax

D = 3584
HQ = 16
KV = 4
DH = 128
BUCKET = 384
SRC = 576
N_DP = 8
N_SEQ = 4


def plan_tables(key):
    pairing_key = jax.random.fold_in(key, 11)
    length_key = jax.random.fold_in(key, 12)
    shuffle_key = jax.random.fold_in(key, 13)
    half_bucket = BUCKET // 2
    bucket_sizes = jnp.array([BUCKET, half_bucket, half_bucket], jnp.int32)
    pairing = jax.random.permutation(pairing_key, N_DP).astype(jnp.int32)
    pair_count = N_DP // 2
    first_lengths = jax.random.randint(length_key, (pair_count, 3), bucket_sizes // 2, bucket_sizes + 1).astype(jnp.int32)
    first_lengths = first_lengths.at[0].set(bucket_sizes)
    second_lengths = (3 * bucket_sizes // 2 - first_lengths).astype(jnp.int32)
    lengths = jnp.zeros((N_DP, 3), jnp.int32).at[pairing[0::2]].set(first_lengths).at[pairing[1::2]].set(second_lengths)
    local_slot = jnp.arange(2 * BUCKET, dtype=jnp.int32)
    bucket_id = (local_slot >= BUCKET).astype(jnp.int32) + (local_slot >= BUCKET + half_bucket).astype(jnp.int32)
    starts = jnp.array([0, BUCKET, BUCKET + half_bucket], jnp.int32)
    offset = local_slot - starts[bucket_id]
    filled = (offset[None, :] < lengths[:, bucket_id]).reshape(-1).astype(jnp.int32)
    order_index = (jnp.cumsum(filled) - 1).astype(jnp.int32)
    sender = order_index % N_DP
    within = jnp.clip(order_index // N_DP, 0, SRC - 1)
    sender_keys = jax.random.split(shuffle_key, N_DP)
    shuffles = jax.vmap(lambda one_key: jax.random.permutation(one_key, SRC))(sender_keys).astype(jnp.int32)
    source_row = (sender * SRC + shuffles[sender, within]).astype(jnp.int32)
    target = jnp.where(filled > 0, source_row, N_DP * SRC)
    global_slot = jnp.arange(N_DP * 2 * BUCKET, dtype=jnp.int32)
    dest = jnp.zeros((N_DP * SRC,), jnp.int32).at[target].set(global_slot, mode='drop')
    return (lengths, dest)


def draw_sample_tokens(key, part):
    return plan_tables(key)[0]


def draw_dest_slot(key, part):
    return plan_tables(key)[1]


def draw_loss_mask(key, part):
    row_total = N_DP * SRC
    row_ids = jnp.arange(row_total, dtype=jnp.int32)
    sender = row_ids // SRC
    level = jax.random.randint(jax.random.fold_in(key, 22), (), 15, 86).astype(jnp.int32)
    jitter = jax.random.randint(jax.random.fold_in(key, 23), (N_DP,), 50, 151).astype(jnp.int32)
    ramp = N_DP - 1 + 2 * sender
    threshold = level * ramp * jitter[sender]
    drawn = jax.random.randint(jax.random.fold_in(key, 21), (row_total,), 0, 100 * (3 * N_DP - 3) * 150)
    chosen = (drawn < threshold) | (row_ids % SRC == 0)
    return chosen.astype(jnp.int32)


def with_ends(values, key, low, high):
    dims = values.shape
    index_at = [jax.random.randint(jax.random.fold_in(key, axis), (), 0, dims[axis]) for axis in range(len(dims))]
    values = values.at[tuple(index_at)].set(low)
    longest = dims.index(max(dims))
    index_at[longest] = (index_at[longest] + 1) % dims[longest]
    return values.at[tuple(index_at)].set(high)


def block_levels(own_key, extent, shards, smallest, top_value):
    level, own = 1.0, jax.random.fold_in(own_key, 6)
    for position, parts in shards:
        draws = jnp.exp(jax.random.uniform(jax.random.fold_in(own, position), (parts,), jnp.float32, smallest / len(shards), top_value / len(shards)))
        level = level * jnp.repeat(draws, extent[position] // parts).reshape([-1 if axis == position else 1 for axis in range(len(extent))])
    return level


def bell_draw(own_key, shape, spread, bound, cuts=(), held_as=jnp.bfloat16):
    level = block_levels(own_key, shape, cuts, -0.22, 0.18) if cuts else 1.0
    entries = jax.random.normal(own_key, shape, jnp.float32) * spread * level
    return jnp.minimum(jnp.maximum(entries, -bound), bound).astype(held_as)


def setup_inputs(seed: int = 0) -> dict:
    streams_of = jax.random.split(jax.random.key(seed), 14)
    tokens = bell_draw(streams_of[0], (N_DP * SRC, D), 1.0, 6.0, ((0, 8),))
    positions = with_ends(jax.random.randint(streams_of[1], (3, N_DP * SRC), 0, 2048), jax.random.fold_in(streams_of[1], 1), 0, 2047).astype(jnp.int32)
    loss_mask = draw_loss_mask(jax.random.fold_in(streams_of[13], 71), 0)
    sample_tokens = draw_sample_tokens(jax.random.fold_in(streams_of[13], 71), 0)
    dest_slot = draw_dest_slot(jax.random.fold_in(streams_of[13], 71), 0)
    norm_gain = jnp.clip(1.0 + 0.1 * jax.random.normal(streams_of[5], (D,), jnp.float32), 0.5, 1.5)
    q_weight = bell_draw(streams_of[6], (D, HQ * DH), D ** -0.5, 0.09375, ((1, 4),))
    k_weight = bell_draw(streams_of[7], (D, KV * DH), D ** -0.5, 0.09375, ((1, 4),))
    v_weight = bell_draw(streams_of[8], (D, KV * DH), D ** -0.5, 0.09375, ((1, 4),))
    q_bias = bell_draw(streams_of[9], (HQ * DH,), 0.5, 3.0, ((0, 4),), jnp.float32)
    k_bias = bell_draw(streams_of[10], (KV * DH,), 0.5, 3.0, ((0, 4),), jnp.float32)
    v_bias = bell_draw(streams_of[11], (KV * DH,), 0.5, 3.0, ((0, 4),), jnp.float32)
    o_weight = bell_draw(streams_of[12], (HQ * DH, D), (HQ * DH) ** -0.5, 0.125, ((0, 4),))
    return {"tokens": tokens, "positions": positions, "loss_mask": loss_mask, "sample_tokens": sample_tokens, "dest_slot": dest_slot, "norm_gain": norm_gain, "q_weight": q_weight, "k_weight": k_weight, "v_weight": v_weight, "q_bias": q_bias, "k_bias": k_bias, "v_bias": v_bias, "o_weight": o_weight}


NORM_EPSILON = 1e-06
ROPE_BASE = 1000000.0

def rms_norm(rows_in, gain):
    widened = rows_in.astype(jnp.float32)
    mean_square = lax.optimization_barrier(jnp.mean(widened * widened, axis=-1, keepdims=True))
    return (widened * lax.rsqrt(mean_square + NORM_EPSILON) * gain).astype(jnp.bfloat16)

def rotary_tables(position_ids, head_size):
    half_size = head_size // 2
    pair_index = jnp.arange(half_size, dtype=jnp.int32)
    inv_freq = jnp.exp(pair_index.astype(jnp.float32) * (-2.0 * math.log(ROPE_BASE) / head_size))
    time_limit = head_size // 8
    height_limit = time_limit + 3 * head_size // 16
    chosen = jnp.where(pair_index[None, :] < time_limit, position_ids[0][:, None], jnp.where(pair_index[None, :] < height_limit, position_ids[1][:, None], position_ids[2][:, None]))
    angles = chosen.astype(jnp.float32) * inv_freq[None, :]
    return (jnp.cos(angles), jnp.sin(angles))

def rotate(heads_in, cosine, sine_part):
    half_size = heads_in.shape[-1] // 2
    first_half = heads_in[..., :half_size]
    second_half = heads_in[..., half_size:]
    cosine = cosine[:, None, :]
    sine_part = sine_part[:, None, :]
    return jnp.concatenate([first_half * cosine - second_half * sine_part, second_half * cosine + first_half * sine_part], axis=-1)

def attend_group(queries, key_rows, value_rows, lengths):
    block_count = queries.shape[0]
    row_count = queries.shape[1]
    scores = jnp.einsum('bqagd,bkad->bagqk', queries.astype(jnp.float32), key_rows.astype(jnp.float32)) * (1.0 / math.sqrt(DH))
    places = jnp.arange(row_count, dtype=jnp.int32)
    allowed = (places[:, None] >= places[None, :])[None] & (places[None, None, :] < lengths[:, None, None])
    scores = jnp.where(allowed[:, None, None], scores, -1e+30)
    weights = jax.nn.softmax(scores, axis=-1).astype(jnp.bfloat16)
    context = jnp.einsum('bagqk,bkad->bqagd', weights.astype(jnp.float32), value_rows.astype(jnp.float32))
    live_rows = places[None, :] < lengths[:, None]
    context = jnp.where(live_rows[:, :, None, None, None], context, 0.0).astype(jnp.bfloat16)
    return context.reshape(block_count * row_count, -1)

def attend_buckets(q_rows, k_rows, v_rows, lengths, kv_count, group_size):
    half_bucket = BUCKET // 2
    first_part = attend_group(q_rows[:BUCKET].reshape(1, BUCKET, kv_count, group_size, DH), k_rows[:BUCKET].reshape(1, BUCKET, kv_count, DH), v_rows[:BUCKET].reshape(1, BUCKET, kv_count, DH), lengths[:1])
    second_part = attend_group(q_rows[BUCKET:].reshape(2, half_bucket, kv_count, group_size, DH), k_rows[BUCKET:].reshape(2, half_bucket, kv_count, DH), v_rows[BUCKET:].reshape(2, half_bucket, kv_count, DH), lengths[1:])
    return jnp.concatenate([first_part, second_part], axis=0)

def reference(tokens, positions, loss_mask, sample_tokens, dest_slot, norm_gain, q_weight, k_weight, v_weight, q_bias, k_bias, v_bias, o_weight):
    peer_count = sample_tokens.shape[0]
    slot_count = 2 * BUCKET
    total_slots = peer_count * slot_count
    head_count = q_weight.shape[1] // DH
    kv_count = k_weight.shape[1] // DH
    group_size = head_count // kv_count
    normed = rms_norm(tokens, norm_gain)
    queries = (jnp.dot(normed, q_weight, preferred_element_type=jnp.float32) + q_bias).astype(jnp.bfloat16)
    key_rows = (jnp.dot(normed, k_weight, preferred_element_type=jnp.float32) + k_bias).astype(jnp.bfloat16)
    value_rows = (jnp.dot(normed, v_weight, preferred_element_type=jnp.float32) + v_bias).astype(jnp.bfloat16)
    cosine, sine_part = rotary_tables(positions, DH)
    queries = rotate(queries.astype(jnp.float32).reshape(-1, head_count, DH), cosine, sine_part).astype(jnp.bfloat16)
    key_rows = rotate(key_rows.astype(jnp.float32).reshape(-1, kv_count, DH), cosine, sine_part).astype(jnp.bfloat16)
    q_slots = jnp.zeros((total_slots, head_count * DH), jnp.bfloat16).at[dest_slot].set(queries.reshape(-1, head_count * DH))
    k_slots = jnp.zeros((total_slots, kv_count * DH), jnp.bfloat16).at[dest_slot].set(key_rows.reshape(-1, kv_count * DH))
    v_slots = jnp.zeros((total_slots, kv_count * DH), jnp.bfloat16).at[dest_slot].set(value_rows)

    def attend(inputs):
        q_rows, k_rows, v_rows, lengths = inputs
        return attend_buckets(q_rows, k_rows, v_rows, lengths, kv_count, group_size)
    context = lax.map(attend, (q_slots.reshape(peer_count, slot_count, head_count * DH), k_slots.reshape(peer_count, slot_count, kv_count * DH), v_slots.reshape(peer_count, slot_count, kv_count * DH), sample_tokens))
    context = context.reshape(total_slots, head_count * DH)
    slice_width = head_count * DH // N_SEQ
    head_total = jnp.zeros((total_slots, tokens.shape[1]), jnp.float32)
    for group_index in range(N_SEQ):
        partial_value = jnp.dot(context[:, group_index * slice_width:(group_index + 1) * slice_width], o_weight[group_index * slice_width:(group_index + 1) * slice_width], preferred_element_type=jnp.float32).astype(jnp.bfloat16)
        head_total = head_total + partial_value.astype(jnp.float32)
    mixed = head_total.astype(jnp.bfloat16)
    mask_float = loss_mask.astype(jnp.float32)
    token_count = jnp.sum(mask_float)
    row_scale = tokens.shape[0] / token_count
    token_weight = jnp.zeros((total_slots,), jnp.float32).at[dest_slot].set(mask_float * row_scale)
    return (mixed, token_weight)
```

```python
import functools
import math

import jax
import jax.numpy as jnp
from jax import lax
from jax.experimental import pallas as pl
from jax.experimental.pallas import tpu as pltpu
from jax.sharding import PartitionSpec as P

DH = 128
BUCKET = 384
LANES = 128

NORM_EPSILON = 1e-06
ROPE_BASE = 1000000.0
F32 = jnp.float32
BF16 = jnp.bfloat16


def rotary_tables(position_ids, head_size):
    half_size = head_size // 2
    pair_index = jnp.arange(head_size, dtype=jnp.int32) % half_size
    inv_freq = jnp.exp(pair_index.astype(F32) * (-2.0 * math.log(ROPE_BASE) / head_size))
    time_limit = head_size // 8
    height_limit = time_limit + 3 * head_size // 16
    chosen = jnp.where(
        pair_index[None, :] < time_limit,
        position_ids[0][:, None],
        jnp.where(
            pair_index[None, :] < height_limit, position_ids[1][:, None], position_ids[2][:, None]
        ),
    )
    angles = chosen.astype(F32) * inv_freq[None, :]
    sign = jnp.where(jnp.arange(head_size) < half_size, -1.0, 1.0).astype(F32)
    return (jnp.cos(angles), jnp.sin(angles) * sign[None, :])


def iota(shape, axis):
    return lax.broadcasted_iota(jnp.int32, shape, axis)


def project_kernel(
    peers, slot_count, room, group, head_count, depth,
    tok_ref, gain_ref, qw_ref, kw_ref, vw_ref, bias_ref, cos_ref, sin_ref, slot_ref, mask_ref,
    packed_ref, info_ref, acc, squares, turned,
):
    step = pl.program_id(0)
    rows = tok_ref.shape[0]
    width = acc.shape[1]

    @pl.when(step == 0)
    def _():
        acc[...] = jnp.zeros_like(acc)
        squares[...] = jnp.zeros_like(squares)

    x = tok_ref[...].astype(F32)
    sq = x * x
    part = sq[:, :LANES]
    for i in range(1, x.shape[1] // LANES):
        part = part + sq[:, i * LANES : (i + 1) * LANES]
    squares[...] += part
    scaled = (x * gain_ref[...]).astype(BF16)
    weights = jnp.concatenate([qw_ref[...], kw_ref[...], vw_ref[...]], axis=1)
    acc[...] += jnp.dot(scaled, weights, preferred_element_type=F32)

    @pl.when(step == pl.num_programs(0) - 1)
    def _():
        mean_square = jnp.sum(squares[...], axis=1, keepdims=True) * (1.0 / depth)
        inverse = lax.rsqrt(mean_square + NORM_EPSILON)
        cosine = cos_ref[...]
        sine = sin_ref[...]
        for h in range(width // DH):
            cols = slice(h * DH, (h + 1) * DH)
            head = (acc[:, cols] * inverse + bias_ref[:, cols]).astype(BF16)
            if h < head_count:
                wide = head.astype(F32)
                head = (wide * cosine + pltpu.roll(wide, DH // 2, 1) * sine).astype(BF16)
            turned[:, cols] = head
        slots = slot_ref[...]
        peer = slots // slot_count
        local = slots - peer * slot_count + 1
        mask = mask_ref[...].astype(F32)
        mask_sum = jnp.sum(mask, axis=1, keepdims=True)
        hot = jnp.where(iota((peers, rows), 0) == peer, 1.0, 0.0)
        earlier = jnp.where(iota((rows, rows), 0) < iota((rows, rows), 1), 1.0, 0.0).astype(BF16)
        counts = jnp.dot(hot.astype(BF16), earlier, preferred_element_type=F32)
        rank = jnp.sum(hot * counts, axis=0, keepdims=True).astype(jnp.int32)
        place = peer * LANES + rank
        high = local // 32
        kind = iota((8, rows), 0)
        facts = jnp.where(
            kind == 0,
            high.astype(F32),
            jnp.where(
                kind == 1, (local - high * 32).astype(F32), jnp.where(kind == 2, mask, 0.0)
            ),
        ).astype(BF16)
        values = turned[...]
        span = group * LANES
        for g in range(peers // group):
            select = jnp.where(iota((span, rows), 0) + g * span == place, 1.0, 0.0).astype(BF16)
            moved = jnp.dot(select, values, preferred_element_type=F32).astype(BF16)
            told = lax.dot_general(
                facts, select, (((1,), (1,)), ((), ())), preferred_element_type=F32
            )
            told = jnp.where(iota(told.shape, 0) == 3, mask_sum, told)
            for p in range(group):
                packed_ref[g * group + p] = moved[p * LANES : p * LANES + room]
                info_ref[g * group + p] = told[:, p * LANES : (p + 1) * LANES]


def attend(kv_slots, lengths, head_count, ctx):
    start = 0
    scale = 1.0 / math.sqrt(DH)
    for size, length in zip((BUCKET, BUCKET // 2, BUCKET // 2), lengths):
        rows = slice(start, start + size)
        key = kv_slots[rows, head_count * DH : (head_count + 1) * DH]
        value = kv_slots[rows, (head_count + 1) * DH : (head_count + 2) * DH]
        q_at, k_at = iota((size, size), 0), iota((size, size), 1)
        allowed = (q_at >= k_at) & (k_at < length)
        live = iota((size, DH), 0) < length
        for h in range(head_count):
            cols = slice(h * DH, (h + 1) * DH)
            scores = lax.dot_general(
                kv_slots[rows, cols], key, (((1,), (1,)), ((), ())), preferred_element_type=F32
            )
            scores = jnp.where(allowed, scores * scale, -1e30)
            top = jnp.max(scores, axis=1, keepdims=True)
            weights = jnp.exp(scores - top)
            total = jnp.sum(weights, axis=1, keepdims=True)
            out = jnp.dot(weights.astype(BF16), value, preferred_element_type=F32) / total
            ctx[rows, cols] = jnp.where(live, out, 0.0).astype(BF16)
        start += size


def exchange_kernel(
    peers, group, seq_count, source_rows, head_count, chunk,
    packed_ref, info_ref, tokens_ref, ow_hbm,
    mixed_ref, weight_ref,
    got, got_info, select, padded, slots, ctx, ow, own,
    near_out, near_in, mine_out, mine_in, far_out, far_in,
    data_send, data_recv, info_send, info_recv, near_send, near_recv,
    mine_send, mine_recv, far_send, far_recv, ow_sem,
):
    me = lax.axis_index("dp")
    seat = lax.axis_index("seq")
    half = seat // 2
    core = seat % 2
    partner = half * 2 + (1 - core)
    across = (1 - half) * 2 + core
    room = packed_ref.shape[1]
    slot_count = slots.shape[0]
    part = slot_count // seq_count
    chunks = ow.shape[1] // chunk

    load = pltpu.make_async_copy(ow_hbm, ow, ow_sem)
    load.start()
    barrier = pltpu.get_barrier_semaphore()
    for d in range(1, peers):
        pl.semaphore_signal(barrier, inc=1, device_id={"dp": (me + d) % peers})
    pl.semaphore_signal(barrier, inc=1, device_id={"seq": partner})
    pl.semaphore_signal(barrier, inc=1, device_id={"seq": across})
    pl.semaphore_wait(barrier, peers + 1)

    def sends(d):
        to = (me + d) % peers
        return (
            pltpu.make_async_remote_copy(
                info_ref.at[to], got_info.at[me], info_send.at[d], info_recv.at[d],
                device_id={"dp": to},
            ),
            pltpu.make_async_remote_copy(
                packed_ref.at[to], got.at[me], data_send.at[d], data_recv.at[d],
                device_id={"dp": to},
            ),
        )

    for d in range(1, peers):
        for copy in sends(d):
            copy.start()
    got[me] = packed_ref[me]
    got_info[me] = info_ref[me]
    padded[...] = jnp.zeros_like(padded)
    for d in range(1, peers):
        for copy in sends(d):
            copy.wait()

    count = jnp.zeros((1, LANES), F32)
    seen = jnp.zeros((8, part), F32)
    placed = jnp.zeros(slots.shape, F32)
    slot_at = iota((slot_count, LANES), 0).astype(F32)
    for g in range(peers // group):
        facts = []
        for p in range(group):
            told = got_info[g * group + p]
            facts.append(told)
            count = count + told[3:4]
            local = told[0:1] * 32.0 + told[1:2] - 1.0
            select[:, p * LANES : (p + 1) * LANES] = jnp.where(
                slot_at == local, 1.0, 0.0
            ).astype(BF16)
            padded[p * LANES : p * LANES + room, :] = got[g * group + p]
        flags = jnp.concatenate(facts, axis=1).astype(BF16)
        own_select = select[pl.ds(pl.multiple_of(seat * part, part), part), :]
        seen = seen + lax.dot_general(
            flags, own_select, (((1,), (1,)), ((), ())), preferred_element_type=F32
        )
        placed = placed + jnp.dot(select[...], padded[...], preferred_element_type=F32)
    slots[...] = placed.astype(BF16)
    weight_ref[...] = seen[2:3] * ((peers * source_rows) / count[:, :1])

    lengths = [tokens_ref[me, i] for i in range(3)]
    attend(slots, lengths, head_count, ctx)
    load.wait()

    def block(index):
        return ctx[pl.ds(pl.multiple_of(index * part, part), part), :]

    def near_copy(j):
        return pltpu.make_async_remote_copy(
            near_out.at[j], near_in.at[j], near_send.at[j], near_recv.at[j],
            device_id={"seq": partner},
        )

    def mine_copy(j):
        return pltpu.make_async_remote_copy(
            mine_out.at[j], mine_in.at[j], mine_send.at[j], mine_recv.at[j],
            device_id={"seq": partner},
        )

    def far_copy(j):
        return pltpu.make_async_remote_copy(
            far_out.at[j], far_in.at[j], far_send.at[j], far_recv.at[j],
            device_id={"seq": across},
        )

    held = [None] * chunks

    def forward(j):
        near_copy(j).wait()
        far_out[j] = (held[j] + near_in[j].astype(F32)).astype(BF16)
        far_copy(j).start()

    for j in range(chunks):
        w = ow[:, j * chunk : (j + 1) * chunk]
        near_out[j] = jnp.dot(
            block((1 - half) * 2 + (1 - core)), w, preferred_element_type=F32
        ).astype(BF16)
        near_copy(j).start()
        held[j] = jnp.dot(block(across), w, preferred_element_type=F32)
        if j > 0:
            forward(j - 1)
    forward(chunks - 1)
    for j in range(chunks):
        w = ow[:, j * chunk : (j + 1) * chunk]
        mine_out[j] = jnp.dot(block(partner), w, preferred_element_type=F32).astype(BF16)
        mine_copy(j).start()
        own[:, j * chunk : (j + 1) * chunk] = jnp.dot(
            block(seat), w, preferred_element_type=F32
        )
    for j in range(chunks):
        mine_copy(j).wait()
        cols = slice(j * chunk, (j + 1) * chunk)
        own[:, cols] += mine_in[j].astype(F32)
    for j in range(chunks):
        far_copy(j).wait()
        cols = slice(j * chunk, (j + 1) * chunk)
        mixed_ref[:, cols] = (own[:, cols] + far_in[j].astype(F32)).astype(BF16)


def per_device(
    tokens, positions, loss_mask, sample_tokens, dest_slot, norm_gain,
    q_weight, k_weight, v_weight, q_bias, k_bias, v_bias, o_weight,
):
    peers = lax.axis_size("dp")
    seq_count = lax.axis_size("seq")
    rows, depth = tokens.shape
    slot_count = 2 * BUCKET
    room = -(-(slot_count // peers) // 16) * 16
    group = math.gcd(peers, 8)
    q_heads = q_weight.shape[1] // DH
    kv_heads = k_weight.shape[1] // DH
    width = (q_heads + 2 * kv_heads) * DH
    chunk = math.gcd(depth, 512)
    part = slot_count // seq_count
    out_width = o_weight.shape[1]
    out_chunk = math.gcd(out_width, 512)
    out_chunks = out_width // out_chunk
    cosine, sine = rotary_tables(positions, DH)
    bias = jnp.concatenate([q_bias, k_bias, v_bias])[None, :]
    whole = lambda *shape: pl.BlockSpec(shape, lambda k: (0,) * len(shape))
    packed, info = pl.pallas_call(
        functools.partial(
            project_kernel, peers, slot_count, room, group, q_heads + kv_heads, depth
        ),
        grid=(depth // chunk,),
        in_specs=[
            pl.BlockSpec((rows, chunk), lambda k: (0, k)),
            pl.BlockSpec((1, chunk), lambda k: (0, k)),
            pl.BlockSpec((chunk, q_heads * DH), lambda k: (k, 0)),
            pl.BlockSpec((chunk, kv_heads * DH), lambda k: (k, 0)),
            pl.BlockSpec((chunk, kv_heads * DH), lambda k: (k, 0)),
            whole(1, width),
            whole(rows, DH),
            whole(rows, DH),
            whole(1, rows),
            whole(1, rows),
        ],
        out_specs=[whole(peers, room, width), whole(peers, 8, LANES)],
        out_shape=[
            jax.ShapeDtypeStruct((peers, room, width), BF16),
            jax.ShapeDtypeStruct((peers, 8, LANES), F32),
        ],
        scratch_shapes=[
            pltpu.VMEM((rows, width), F32),
            pltpu.VMEM((rows, LANES), F32),
            pltpu.VMEM((rows, width), BF16),
        ],
        compiler_params=pltpu.CompilerParams(vmem_limit_bytes=56 * 2**20),
    )(
        tokens, norm_gain[None, :], q_weight, k_weight, v_weight, bias, cosine, sine,
        dest_slot[None, :], loss_mask[None, :],
    )
    vmem = pl.BlockSpec(memory_space=pltpu.VMEM)
    piece = pltpu.VMEM((out_chunks, part, out_chunk), BF16)
    dma = pltpu.SemaphoreType.DMA
    mixed, weight = pl.pallas_call(
        functools.partial(
            exchange_kernel, peers, group, seq_count, rows, q_heads, out_chunk
        ),
        in_specs=[
            vmem,
            vmem,
            pl.BlockSpec(memory_space=pltpu.SMEM),
            pl.BlockSpec(memory_space=pl.ANY),
        ],
        out_specs=[vmem, vmem],
        out_shape=[
            jax.ShapeDtypeStruct((part, out_width), BF16),
            jax.ShapeDtypeStruct((1, part), F32),
        ],
        scratch_shapes=[
            pltpu.VMEM((peers, room, width), BF16),
            pltpu.VMEM((peers, 8, LANES), F32),
            pltpu.VMEM((slot_count, group * LANES), BF16),
            pltpu.VMEM((group * LANES, width), BF16),
            pltpu.VMEM((slot_count, width), BF16),
            pltpu.VMEM((slot_count, q_heads * DH), BF16),
            pltpu.VMEM(o_weight.shape, BF16),
            pltpu.VMEM((part, out_width), F32),
            piece, piece, piece, piece, piece, piece,
            dma((peers,)), dma((peers,)), dma((peers,)), dma((peers,)),
            dma((out_chunks,)), dma((out_chunks,)), dma((out_chunks,)),
            dma((out_chunks,)), dma((out_chunks,)), dma((out_chunks,)),
            dma,
        ],
        compiler_params=pltpu.CompilerParams(
            collective_id=0, has_side_effects=True, vmem_limit_bytes=56 * 2**20
        ),
    )(packed, info, sample_tokens, o_weight)
    return (mixed, weight.reshape(part))


def solution(mesh):
    return jax.shard_map(
        per_device,
        mesh=mesh,
        in_specs=(
            P("dp", None),
            P(None, "dp"),
            P("dp"),
            P(),
            P("dp"),
            P(),
            P(None, "seq"),
            P(None, "seq"),
            P(None, "seq"),
            P("seq"),
            P("seq"),
            P("seq"),
            P("seq", None),
        ),
        out_specs=(P(("dp", "seq"), None), P(("dp", "seq"))),
        check_vma=False,
    )
```

```python
import functools
import math

import jax
import jax.numpy as jnp
from jax import lax
from jax.experimental import pallas as pl
from jax.experimental.pallas import tpu as pltpu
from jax.sharding import PartitionSpec as P

DH = 128
BUCKET = 384
LANES = 128

NORM_EPSILON = 1e-06
ROPE_BASE = 1000000.0
F32 = jnp.float32
BF16 = jnp.bfloat16


def rotary_tables(position_ids, head_size):
    half_size = head_size // 2
    pair_index = jnp.arange(head_size, dtype=jnp.int32) % half_size
    inv_freq = jnp.exp(pair_index.astype(F32) * (-2.0 * math.log(ROPE_BASE) / head_size))
    time_limit = head_size // 8
    height_limit = time_limit + 3 * head_size // 16
    chosen = jnp.where(
        pair_index[None, :] < time_limit,
        position_ids[0][:, None],
        jnp.where(
            pair_index[None, :] < height_limit, position_ids[1][:, None], position_ids[2][:, None]
        ),
    )
    angles = chosen.astype(F32) * inv_freq[None, :]
    sign = jnp.where(jnp.arange(head_size) < half_size, -1.0, 1.0).astype(F32)
    return (jnp.cos(angles), jnp.sin(angles) * sign[None, :])


def iota(shape, axis):
    return lax.broadcasted_iota(jnp.int32, shape, axis)


def pack_plan(peers, slot_count, group, slot_ref, mask_ref, select_out, info_out):
    rows = slot_ref.shape[0]
    slots = slot_ref[...][None, :]
    peer = slots // slot_count
    local = slots - peer * slot_count + 1
    mask = mask_ref[...][None, :].astype(F32)
    mask_sum = jnp.sum(mask, axis=1, keepdims=True)
    hot = jnp.where(iota((peers, rows), 0) == peer, 1.0, 0.0)
    earlier = jnp.where(iota((rows, rows), 0) < iota((rows, rows), 1), 1.0, 0.0).astype(BF16)
    counts = jnp.dot(hot.astype(BF16), earlier, preferred_element_type=F32)
    rank = jnp.sum(hot * counts, axis=0, keepdims=True).astype(jnp.int32)
    place = peer * LANES + rank
    high = local // 32
    kind = iota((8, rows), 0)
    facts = jnp.where(
        kind == 0,
        high.astype(F32),
        jnp.where(kind == 1, (local - high * 32).astype(F32), jnp.where(kind == 2, mask, 0.0)),
    ).astype(BF16)
    span = group * LANES
    for g in range(peers // group):
        select = jnp.where(iota((span, rows), 0) + g * span == place, 1.0, 0.0).astype(BF16)
        select_out[g * span : (g + 1) * span, :] = select
        told = lax.dot_general(facts, select, (((1,), (1,)), ((), ())), preferred_element_type=F32)
        told = jnp.where(iota(told.shape, 0) == 3, mask_sum, told)
        for p in range(group):
            info_out[g * group + p] = told[:, p * LANES : (p + 1) * LANES]


def attend(q_slots, kv_slots, lengths, heads, per_kv, kv_count, ctx):
    start = 0
    scale = 1.0 / math.sqrt(DH)
    for size, length in zip((BUCKET, BUCKET // 2, BUCKET // 2), lengths):
        rows = slice(start, start + size)
        q_at, k_at = iota((size, size), 0), iota((size, size), 1)
        allowed = (q_at >= k_at) & (k_at < length)
        live = iota((size, DH), 0) < length
        for h in heads:
            pair = h // per_kv
            key = kv_slots[rows, pair * DH : (pair + 1) * DH]
            value = kv_slots[rows, (kv_count + pair) * DH : (kv_count + pair + 1) * DH]
            cols = slice(h * DH, (h + 1) * DH)
            scores = lax.dot_general(
                q_slots[rows, cols], key, (((1,), (1,)), ((), ())), preferred_element_type=F32
            )
            scores = jnp.where(allowed, scores * scale, -1e30)
            top = jnp.max(scores, axis=1, keepdims=True)
            weights = jnp.exp(scores - top)
            total = jnp.sum(weights, axis=1, keepdims=True)
            out = jnp.dot(weights.astype(BF16), value, preferred_element_type=F32) / total
            ctx[rows, cols] = jnp.where(live, out, 0.0).astype(BF16)
        start += size


def layer_kernel(
    peers, group, seq_count, q_heads, kv_heads, chunk, room, strips,
    tok_hbm, gain_ref, qw_hbm, kw_hbm, vw_hbm, qb_ref, kb_ref, vb_ref, cos_ref, sin_ref,
    slot_ref, mask_ref, tokens_ref, ow_hbm,
    mixed_ref, weight_ref,
    x, squares, qw, kvw, ow, pick, told_out, got_info, q_out, q_got, kv_out, kv_got,
    select, padded, q_slots, kv_slots, ctx, own,
    near_out, near_in, mine_out, mine_in, far_out, far_in,
    data_send, data_recv, info_send, info_recv, near_send, near_recv,
    mine_send, mine_recv, far_send, far_recv, load_sem,
):
    me = lax.axis_index("dp")
    seat = lax.axis_index("seq")
    half = seat // 2
    core = seat % 2
    partner = half * 2 + (1 - core)
    across = (1 - half) * 2 + core
    rows, depth = x.shape
    slot_count = q_slots.shape[0]
    part = slot_count // seq_count
    chunks = ow.shape[1] // chunk
    strip = rows // strips
    kv_cols = kv_heads * DH

    barrier = pltpu.get_barrier_semaphore()
    for d in range(1, peers):
        pl.semaphore_signal(barrier, inc=1, device_id={"dp": (me + d) % peers})
    pl.semaphore_signal(barrier, inc=1, device_id={"seq": partner})
    pl.semaphore_signal(barrier, inc=1, device_id={"seq": across})
    token_loads = [
        pltpu.make_async_copy(
            tok_hbm.at[i * strip : (i + 1) * strip], x.at[i * strip : (i + 1) * strip],
            load_sem.at[i],
        )
        for i in range(strips)
    ]
    k_load = pltpu.make_async_copy(kw_hbm, kvw.at[:, :kv_cols], load_sem.at[strips])
    v_load = pltpu.make_async_copy(vw_hbm, kvw.at[:, kv_cols:], load_sem.at[strips + 1])
    q_load = pltpu.make_async_copy(qw_hbm, qw, load_sem.at[strips + 2])
    o_load = pltpu.make_async_copy(ow_hbm, ow, load_sem.at[strips + 3])
    for copy in token_loads + [k_load, v_load, q_load, o_load]:
        copy.start()

    pack_plan(peers, slot_count, group, slot_ref, mask_ref, pick, told_out)
    gain = gain_ref[...][None, :]
    for i in range(strips):
        token_loads[i].wait()
        at = slice(i * strip, (i + 1) * strip)
        total = jnp.zeros((strip, LANES), F32)
        for c in range(depth // LANES):
            cols = slice(c * LANES, (c + 1) * LANES)
            wide = x[at, cols].astype(F32)
            total = total + wide * wide
            x[at, cols] = (wide * gain[:, cols]).astype(BF16)
        squares[at, :] = jnp.sum(total, axis=1, keepdims=True)
    inverse = lax.rsqrt(squares[...] * (1.0 / depth) + NORM_EPSILON)

    def info_copy(d):
        to = (me + d) % peers
        return pltpu.make_async_remote_copy(
            told_out.at[to], got_info.at[me], info_send.at[d], info_recv.at[d],
            device_id={"dp": to},
        )

    def data_copy(stage, d):
        to = (me + d) % peers
        source, target = (kv_out, kv_got) if stage == 0 else (q_out, q_got)
        if stage > 0:
            source, target = source.at[stage - 1], target.at[stage - 1]
        return pltpu.make_async_remote_copy(
            source.at[to], target.at[me], data_send.at[stage, d], data_recv.at[stage, d],
            device_id={"dp": to},
        )

    def turn(wide):
        return wide * cos_ref[...] + pltpu.roll(wide, DH // 2, 1) * sin_ref[...]

    def pack(stage, values):
        span = group * LANES
        target, kept = (kv_out, kv_got) if stage == 0 else (q_out, q_got)
        if stage > 0:
            target, kept = target.at[stage - 1], kept.at[stage - 1]
        for g in range(peers // group):
            moved = jnp.dot(
                pick[g * span : (g + 1) * span, :], values, preferred_element_type=F32
            ).astype(BF16)
            for p in range(group):
                target[g * group + p] = moved[p * LANES : p * LANES + room]
        for d in range(1, peers):
            data_copy(stage, d).start()
        kept[me] = target[me]

    pl.semaphore_wait(barrier, peers + 1)
    for d in range(1, peers):
        info_copy(d).start()
    got_info[me] = told_out[me]
    k_load.wait()
    v_load.wait()
    product = jnp.dot(x[...], kvw[...], preferred_element_type=F32)
    pieces = []
    for h in range(2 * kv_heads):
        bias_ref, at = (kb_ref, h) if h < kv_heads else (vb_ref, h - kv_heads)
        bias = bias_ref[at * DH : (at + 1) * DH][None, :]
        head = (product[:, h * DH : (h + 1) * DH] * inverse + bias).astype(BF16)
        if h < kv_heads:
            head = turn(head.astype(F32)).astype(BF16)
        pieces.append(head)
    pack(0, jnp.concatenate(pieces, axis=1))
    q_load.wait()
    q_stages = q_out.shape[0]
    per_stage = q_heads // q_stages
    for stage in range(q_stages):
        cols = slice(stage * per_stage * DH, (stage + 1) * per_stage * DH)
        product = jnp.dot(x[...], qw[:, cols], preferred_element_type=F32)
        pieces = []
        for i in range(per_stage):
            h = stage * per_stage + i
            bias = qb_ref[h * DH : (h + 1) * DH][None, :]
            head = (product[:, i * DH : (i + 1) * DH] * inverse + bias).astype(BF16)
            pieces.append(turn(head.astype(F32)).astype(BF16))
        pack(stage + 1, jnp.concatenate(pieces, axis=1))

    padded[...] = jnp.zeros_like(padded)
    for d in range(1, peers):
        info_copy(d).wait()
    count = jnp.zeros((1, LANES), F32)
    slot_at = iota((slot_count, LANES), 0).astype(F32)
    facts = []
    for p in range(peers):
        told = got_info[p]
        facts.append(told)
        count = count + told[3:4]
        local = told[0:1] * 32.0 + told[1:2] - 1.0
        select[:, p * LANES : (p + 1) * LANES] = jnp.where(slot_at == local, 1.0, 0.0).astype(BF16)
    flags = jnp.concatenate(facts, axis=1).astype(BF16)
    own_select = select[pl.ds(pl.multiple_of(seat * part, part), part), :]
    seen = lax.dot_general(flags, own_select, (((1,), (1,)), ((), ())), preferred_element_type=F32)
    weight_ref[...] = seen[2:3] * ((peers * rows) / count[:, :1])

    def place(stage):
        for d in range(1, peers):
            data_copy(stage, d).wait()
        source = kv_got if stage == 0 else q_got.at[stage - 1]
        width = source.shape[2]
        for p in range(peers):
            padded[p * LANES : p * LANES + room, :width] = source[p]
        return jnp.dot(select[...], padded[:, :width], preferred_element_type=F32).astype(BF16)

    mine = tokens_ref[pl.ds(me, 1), :]
    lengths = [mine[:, i : i + 1] for i in range(3)]
    kv_slots[...] = place(0)
    for stage in range(q_stages):
        cols = slice(stage * per_stage * DH, (stage + 1) * per_stage * DH)
        q_slots[:, cols] = place(stage + 1)
        heads = range(stage * per_stage, (stage + 1) * per_stage)
        attend(q_slots, kv_slots, lengths, heads, q_heads // kv_heads, kv_heads, ctx)
    o_load.wait()

    def block(index):
        return ctx[pl.ds(pl.multiple_of(index * part, part), part), :]

    def near_copy(j):
        return pltpu.make_async_remote_copy(
            near_out.at[j], near_in.at[j], near_send.at[j], near_recv.at[j],
            device_id={"seq": partner},
        )

    def mine_copy(j):
        return pltpu.make_async_remote_copy(
            mine_out.at[j], mine_in.at[j], mine_send.at[j], mine_recv.at[j],
            device_id={"seq": partner},
        )

    def far_copy(j):
        return pltpu.make_async_remote_copy(
            far_out.at[j], far_in.at[j], far_send.at[j], far_recv.at[j],
            device_id={"seq": across},
        )

    held = [None] * chunks

    def forward(j):
        near_copy(j).wait()
        far_out[j] = (held[j] + near_in[j].astype(F32)).astype(BF16)
        far_copy(j).start()

    for j in range(chunks):
        w = ow[:, j * chunk : (j + 1) * chunk]
        near_out[j] = jnp.dot(
            block((1 - half) * 2 + (1 - core)), w, preferred_element_type=F32
        ).astype(BF16)
        near_copy(j).start()
        held[j] = jnp.dot(block(across), w, preferred_element_type=F32)
        if j > 0:
            forward(j - 1)
    forward(chunks - 1)
    for j in range(chunks):
        w = ow[:, j * chunk : (j + 1) * chunk]
        mine_out[j] = jnp.dot(block(partner), w, preferred_element_type=F32).astype(BF16)
        mine_copy(j).start()
        own[:, j * chunk : (j + 1) * chunk] = jnp.dot(
            block(seat), w, preferred_element_type=F32
        )
    for j in range(chunks):
        mine_copy(j).wait()
        cols = slice(j * chunk, (j + 1) * chunk)
        own[:, cols] += mine_in[j].astype(F32)
    for j in range(chunks):
        far_copy(j).wait()
        cols = slice(j * chunk, (j + 1) * chunk)
        mixed_ref[:, cols] = (own[:, cols] + far_in[j].astype(F32)).astype(BF16)


def per_device(
    tokens, positions, loss_mask, sample_tokens, dest_slot, norm_gain,
    q_weight, k_weight, v_weight, q_bias, k_bias, v_bias, o_weight,
):
    peers = lax.axis_size("dp")
    seq_count = lax.axis_size("seq")
    rows, depth = tokens.shape
    slot_count = 2 * BUCKET
    room = -(-(slot_count // peers) // 16) * 16
    group = math.gcd(peers, 8)
    q_heads = q_weight.shape[1] // DH
    kv_heads = k_weight.shape[1] // DH
    per_stage = math.gcd(q_heads, 2)
    stages = q_heads // per_stage
    strips = math.gcd(rows // 16, 4)
    part = slot_count // seq_count
    out_width = o_weight.shape[1]
    chunk = math.gcd(out_width, 512)
    chunks = out_width // chunk
    kv_width = 2 * kv_heads * DH
    q_width = per_stage * DH
    cosine, sine = rotary_tables(positions, DH)
    vmem = pl.BlockSpec(memory_space=pltpu.VMEM)
    hbm = pl.BlockSpec(memory_space=pl.ANY)
    piece = pltpu.VMEM((chunks, part, chunk), BF16)
    dma = pltpu.SemaphoreType.DMA
    mixed, weight = pl.pallas_call(
        functools.partial(
            layer_kernel, peers, group, seq_count, q_heads, kv_heads, chunk, room, strips
        ),
        in_specs=[
            hbm, vmem, hbm, hbm, hbm, vmem, vmem, vmem, vmem, vmem, vmem, vmem, vmem, hbm,
        ],
        out_specs=[vmem, vmem],
        out_shape=[
            jax.ShapeDtypeStruct((part, out_width), BF16),
            jax.ShapeDtypeStruct((1, part), F32),
        ],
        scratch_shapes=[
            pltpu.VMEM((rows, depth), BF16),
            pltpu.VMEM((rows, 1), F32),
            pltpu.VMEM(q_weight.shape, BF16),
            pltpu.VMEM((depth, kv_width), BF16),
            pltpu.VMEM(o_weight.shape, BF16),
            pltpu.VMEM((peers * LANES, rows), BF16),
            pltpu.VMEM((peers, 8, LANES), F32),
            pltpu.VMEM((peers, 8, LANES), F32),
            pltpu.VMEM((stages, peers, room, q_width), BF16),
            pltpu.VMEM((stages, peers, room, q_width), BF16),
            pltpu.VMEM((peers, room, kv_width), BF16),
            pltpu.VMEM((peers, room, kv_width), BF16),
            pltpu.VMEM((slot_count, peers * LANES), BF16),
            pltpu.VMEM((peers * LANES, max(kv_width, q_width)), BF16),
            pltpu.VMEM((slot_count, q_heads * DH), BF16),
            pltpu.VMEM((slot_count, kv_width), BF16),
            pltpu.VMEM((slot_count, q_heads * DH), BF16),
            pltpu.VMEM((part, out_width), F32),
            piece, piece, piece, piece, piece, piece,
            dma((stages + 1, peers)), dma((stages + 1, peers)), dma((peers,)), dma((peers,)),
            dma((chunks,)), dma((chunks,)), dma((chunks,)),
            dma((chunks,)), dma((chunks,)), dma((chunks,)),
            dma((strips + 4,)),
        ],
        compiler_params=pltpu.CompilerParams(
            collective_id=0, has_side_effects=True, vmem_limit_bytes=67043328
        ),
    )(
        tokens, norm_gain, q_weight, k_weight, v_weight, q_bias, k_bias, v_bias, cosine, sine,
        dest_slot, loss_mask, sample_tokens, o_weight,
    )
    return (mixed, weight.reshape(part))


def solution(mesh):
    return jax.shard_map(
        per_device,
        mesh=mesh,
        in_specs=(
            P("dp", None),
            P(None, "dp"),
            P("dp"),
            P(),
            P("dp"),
            P(),
            P(None, "seq"),
            P(None, "seq"),
            P(None, "seq"),
            P("seq"),
            P("seq"),
            P("seq"),
            P("seq", None),
        ),
        out_specs=(P(("dp", "seq"), None), P(("dp", "seq"))),
        check_vma=False,
    )
```

```python
import functools
import math

import jax
import jax.numpy as jnp
from jax import lax
from jax.experimental import pallas as pl
from jax.experimental.pallas import tpu as pltpu
from jax.sharding import PartitionSpec as P

DH = 128
BUCKET = 384
LANES = 128

NORM_EPSILON = 1e-06
ROPE_BASE = 1000000.0
F32 = jnp.float32
BF16 = jnp.bfloat16


def iota(shape, axis):
    return lax.broadcasted_iota(jnp.int32, shape, axis)


def rotary_tables(pos_ref, cos_out, sin_out):
    ids = pos_ref[...]
    rows = ids.shape[1]
    high = ids // 32
    low = ids - high * 32
    kind = iota((8, rows), 0)
    split = jnp.zeros((8, rows), jnp.int32)
    for axis in range(3):
        split = jnp.where(kind == 2 * axis, high[axis : axis + 1], split)
        split = jnp.where(kind == 2 * axis + 1, low[axis : axis + 1], split)
    half_size = DH // 2
    lane, row = iota((8, DH), 1), iota((8, DH), 0)
    pair = lane % half_size
    time_limit = DH // 8
    height_limit = time_limit + 3 * DH // 16
    axis = jnp.where(pair < time_limit, 0, jnp.where(pair < height_limit, 1, 2))
    pick = jnp.where(row == 2 * axis, 32.0, jnp.where(row == 2 * axis + 1, 1.0, 0.0))
    chosen = lax.dot_general(
        split.astype(F32).astype(BF16), pick.astype(BF16), (((0,), (0,)), ((), ())),
        preferred_element_type=F32,
    )
    turn_at = iota((1, DH), 1)
    power = (turn_at % half_size).astype(F32)
    angles = chosen * jnp.exp(power * (-2.0 * math.log(ROPE_BASE) / DH))
    cos_out[...] = jnp.cos(angles)
    sin_out[...] = jnp.sin(angles) * jnp.where(turn_at < half_size, -1.0, 1.0)


def pack_plan(peers, slot_count, group, slot_ref, mask_ref, select_out, info_out):
    rows = slot_ref.shape[0]
    slots = slot_ref[...][None, :]
    peer = slots // slot_count
    local = slots - peer * slot_count + 1
    mask = mask_ref[...][None, :].astype(F32)
    mask_sum = jnp.sum(mask, axis=1, keepdims=True)
    hot = jnp.where(iota((peers, rows), 0) == peer, 1.0, 0.0)
    earlier = jnp.where(iota((rows, rows), 0) < iota((rows, rows), 1), 1.0, 0.0).astype(BF16)
    counts = jnp.dot(hot.astype(BF16), earlier, preferred_element_type=F32)
    rank = jnp.sum(hot * counts, axis=0, keepdims=True).astype(jnp.int32)
    place = peer * LANES + rank
    high = local // 32
    kind = iota((8, rows), 0)
    facts = jnp.where(
        kind == 0,
        high.astype(F32),
        jnp.where(kind == 1, (local - high * 32).astype(F32), jnp.where(kind == 2, mask, 0.0)),
    ).astype(BF16)
    span = group * LANES
    for g in range(peers // group):
        select = jnp.where(iota((span, rows), 0) + g * span == place, 1.0, 0.0).astype(BF16)
        select_out[g * span : (g + 1) * span, :] = select
        told = lax.dot_general(facts, select, (((1,), (1,)), ((), ())), preferred_element_type=F32)
        told = jnp.where(iota(told.shape, 0) == 3, mask_sum, told)
        for p in range(group):
            info_out[g * group + p] = told[:, p * LANES : (p + 1) * LANES]


def attend(q_slots, kv_slots, lengths, heads, per_kv, kv_count, ctx):
    start = 0
    scale = 1.0 / math.sqrt(DH)
    for size, length in zip((BUCKET, BUCKET // 2, BUCKET // 2), lengths):
        rows = slice(start, start + size)
        q_at, k_at = iota((size, size), 0), iota((size, size), 1)
        allowed = (q_at >= k_at) & (k_at < length)
        live = iota((size, DH), 0) < length
        for h in heads:
            pair = h // per_kv
            key = kv_slots[rows, pair * DH : (pair + 1) * DH]
            value = kv_slots[rows, (kv_count + pair) * DH : (kv_count + pair + 1) * DH]
            cols = slice(h * DH, (h + 1) * DH)
            scores = lax.dot_general(
                q_slots[rows, cols], key, (((1,), (1,)), ((), ())), preferred_element_type=F32
            )
            scores = jnp.where(allowed, scores * scale, -1e30)
            top = jnp.max(scores, axis=1, keepdims=True)
            weights = jnp.exp(scores - top)
            total = jnp.sum(weights, axis=1, keepdims=True)
            out = jnp.dot(weights.astype(BF16), value, preferred_element_type=F32) / total
            ctx[rows, cols] = jnp.where(live, out, 0.0).astype(BF16)
        start += size


def layer_kernel(
    peers, group, seq_count, q_heads, kv_heads, chunk, room, strips,
    tok_hbm, gain_ref, qw_hbm, kw_hbm, vw_hbm, qb_ref, kb_ref, vb_ref, pos_ref,
    slot_ref, mask_ref, ow_hbm,
    mixed_ref, weight_ref,
    x, squares, qw, kvw, ow, pick, told_out, got_info, q_out, q_got, kv_out, kv_got,
    select, padded, q_slots, kv_slots, ctx, own,
    near_out, near_in, mine_out, mine_in, far_out, far_in, cos_ref, sin_ref, wide, ctx_all,
    data_send, data_recv, info_send, info_recv, near_send, near_recv,
    mine_send, mine_recv, far_send, far_recv, load_sem, wide_load_sem,
    wide_send, wide_recv, ctx_send, ctx_recv,
):
    me = lax.axis_index("dp")
    seat = lax.axis_index("seq")
    half = seat // 2
    core = seat % 2
    partner = half * 2 + (1 - core)
    across = (1 - half) * 2 + core
    q_stages = q_out.shape[0]
    per_stage = q_heads // q_stages
    rows, depth = x.shape
    slot_count = q_slots.shape[0]
    part = slot_count // seq_count
    wides = wide.shape[1]
    chunks = ow.shape[1] // chunk
    diagonal = (1 - half) * 2 + (1 - core)
    strip = rows // strips
    kv_cols = kv_heads * DH

    barrier = pltpu.get_barrier_semaphore()
    for d in range(1, peers):
        pl.semaphore_signal(barrier, inc=1, device_id={"dp": (me + d) % peers})
    pl.semaphore_signal(barrier, inc=1, device_id={"seq": partner})
    pl.semaphore_signal(barrier, inc=1, device_id={"seq": across})
    pl.semaphore_signal(barrier, inc=1, device_id={"seq": diagonal})
    token_loads = [
        pltpu.make_async_copy(
            tok_hbm.at[i * strip : (i + 1) * strip], x.at[i * strip : (i + 1) * strip],
            load_sem.at[i],
        )
        for i in range(strips)
    ]
    k_load = pltpu.make_async_copy(kw_hbm, kvw.at[:, :kv_cols], load_sem.at[strips])
    v_load = pltpu.make_async_copy(vw_hbm, kvw.at[:, kv_cols:], load_sem.at[strips + 1])
    q_load = pltpu.make_async_copy(qw_hbm, qw, load_sem.at[strips + 2])
    o_load = pltpu.make_async_copy(ow_hbm.at[:, wides * chunk :], ow, load_sem.at[strips + 3])
    wide_loads = [
        pltpu.make_async_copy(
            ow_hbm.at[:, i * chunk : (i + 1) * chunk], wide.at[seat, i], wide_load_sem.at[i]
        )
        for i in range(wides)
    ]
    for copy in token_loads + [k_load, v_load] + wide_loads + [q_load, o_load]:
        copy.start()

    pack_plan(peers, slot_count, group, slot_ref, mask_ref, pick, told_out)
    rotary_tables(pos_ref, cos_ref, sin_ref)
    gain = gain_ref[...][None, :]
    for i in range(strips):
        token_loads[i].wait()
        at = slice(i * strip, (i + 1) * strip)
        total = jnp.zeros((strip, LANES), F32)
        for c in range(depth // LANES):
            cols = slice(c * LANES, (c + 1) * LANES)
            entry = x[at, cols].astype(F32)
            total = total + entry * entry
            x[at, cols] = (entry * gain[:, cols]).astype(BF16)
        squares[at, :] = jnp.sum(total, axis=1, keepdims=True)
    inverse = lax.rsqrt(squares[...] * (1.0 / depth) + NORM_EPSILON)

    def info_copy(d):
        to = (me + d) % peers
        return pltpu.make_async_remote_copy(
            told_out.at[to], got_info.at[me], info_send.at[d], info_recv.at[d],
            device_id={"dp": to},
        )

    def wide_copy(kind, i):
        index = across if kind == 2 else seat
        return pltpu.make_async_remote_copy(
            wide.at[index, i], wide.at[index, i], wide_send.at[kind, i], wide_recv.at[kind, i],
            device_id={"seq": across if kind == 1 else partner},
        )

    def pass_on(i):
        wide_copy(1, i).wait()
        wide_copy(2, i).start()

    def ctx_copy(stage, kind):
        to = (partner, across, diagonal)[kind]
        cols = slice(stage * per_stage * DH, (stage + 1) * per_stage * DH)
        return pltpu.make_async_remote_copy(
            ctx.at[pl.ds(pl.multiple_of(to * part, part), part), cols],
            ctx_all.at[seat, :, cols], ctx_send.at[stage, kind], ctx_recv.at[stage, kind],
            device_id={"seq": to},
        )

    def data_copy(stage, d):
        to = (me + d) % peers
        source, target = (kv_out, kv_got) if stage == 0 else (q_out, q_got)
        if stage > 0:
            source, target = source.at[stage - 1], target.at[stage - 1]
        return pltpu.make_async_remote_copy(
            source.at[to], target.at[me], data_send.at[stage, d], data_recv.at[stage, d],
            device_id={"dp": to},
        )

    def turn(wide):
        return wide * cos_ref[...] + pltpu.roll(wide, DH // 2, 1) * sin_ref[...]

    def pack(stage, values):
        span = group * LANES
        target, kept = (kv_out, kv_got) if stage == 0 else (q_out, q_got)
        if stage > 0:
            target, kept = target.at[stage - 1], kept.at[stage - 1]
        for g in range(peers // group):
            moved = jnp.dot(
                pick[g * span : (g + 1) * span, :], values, preferred_element_type=F32
            ).astype(BF16)
            for p in range(group):
                target[g * group + p] = moved[p * LANES : p * LANES + room]
        for d in range(1, peers):
            data_copy(stage, d).start()
        kept[me] = target[me]

    pl.semaphore_wait(barrier, peers + 2)
    for d in range(1, peers):
        info_copy(d).start()
    got_info[me] = told_out[me]
    for i in range(wides):
        wide_loads[i].wait()
        wide_copy(1, i).start()
        wide_copy(0, i).start()
    k_load.wait()
    v_load.wait()
    product = jnp.dot(x[...], kvw[...], preferred_element_type=F32)
    pieces = []
    for h in range(2 * kv_heads):
        bias_ref, at = (kb_ref, h) if h < kv_heads else (vb_ref, h - kv_heads)
        bias = bias_ref[at * DH : (at + 1) * DH][None, :]
        head = (product[:, h * DH : (h + 1) * DH] * inverse + bias).astype(BF16)
        if h < kv_heads:
            head = turn(head.astype(F32)).astype(BF16)
        pieces.append(head)
    pack(0, jnp.concatenate(pieces, axis=1))
    q_load.wait()
    for stage in range(q_stages):
        cols = slice(stage * per_stage * DH, (stage + 1) * per_stage * DH)
        product = jnp.dot(x[...], qw[:, cols], preferred_element_type=F32)
        pieces = []
        for i in range(per_stage):
            h = stage * per_stage + i
            bias = qb_ref[h * DH : (h + 1) * DH][None, :]
            head = (product[:, i * DH : (i + 1) * DH] * inverse + bias).astype(BF16)
            pieces.append(turn(head.astype(F32)).astype(BF16))
        pack(stage + 1, jnp.concatenate(pieces, axis=1))

    padded[...] = jnp.zeros_like(padded)
    for d in range(1, peers):
        info_copy(d).wait()
    count = jnp.zeros((1, LANES), F32)
    slot_at = iota((slot_count, LANES), 0).astype(F32)
    facts = []
    filled = [jnp.zeros((1, LANES), F32) for _ in range(3)]
    starts = (0, BUCKET, BUCKET + BUCKET // 2, 2 * BUCKET)
    for p in range(peers):
        told = got_info[p]
        facts.append(told)
        count = count + told[3:4]
        local = told[0:1] * 32.0 + told[1:2] - 1.0
        for b in range(3):
            inside = (local >= float(starts[b])) & (local < float(starts[b + 1]))
            filled[b] = filled[b] + jnp.where(inside, 1.0, 0.0)
        select[:, p * LANES : (p + 1) * LANES] = jnp.where(slot_at == local, 1.0, 0.0).astype(BF16)
    flags = jnp.concatenate(facts, axis=1).astype(BF16)
    own_select = select[pl.ds(pl.multiple_of(seat * part, part), part), :]
    seen = lax.dot_general(flags, own_select, (((1,), (1,)), ((), ())), preferred_element_type=F32)
    weight_ref[...] = seen[2:3] * ((peers * rows) / count[:, :1])

    def place(stage):
        for d in range(1, peers):
            data_copy(stage, d).wait()
        source = kv_got if stage == 0 else q_got.at[stage - 1]
        width = source.shape[2]
        for p in range(peers):
            padded[p * LANES : p * LANES + room, :width] = source[p]
        return jnp.dot(select[...], padded[:, :width], preferred_element_type=F32).astype(BF16)

    lengths = [jnp.sum(one, axis=1, keepdims=True).astype(jnp.int32) for one in filled]
    kv_slots[...] = place(0)
    for stage in range(q_stages):
        cols = slice(stage * per_stage * DH, (stage + 1) * per_stage * DH)
        q_slots[:, cols] = place(stage + 1)
        heads = range(stage * per_stage, (stage + 1) * per_stage)
        if stage == 0 and wides > 1:
            pass_on(0)
        attend(q_slots, kv_slots, lengths, heads, q_heads // kv_heads, kv_heads, ctx)
        for kind in range(3):
            ctx_copy(stage, kind).start()
        ctx_all[seat, :, cols] = ctx[pl.ds(pl.multiple_of(seat * part, part), part), cols]
    for i in range(1, wides - 1):
        pass_on(i)
    o_load.wait()

    def block(index):
        return ctx[pl.ds(pl.multiple_of(index * part, part), part), :]

    def near_copy(j):
        return pltpu.make_async_remote_copy(
            near_out.at[j], near_in.at[j], near_send.at[j], near_recv.at[j],
            device_id={"seq": partner},
        )

    def mine_copy(j):
        return pltpu.make_async_remote_copy(
            mine_out.at[j], mine_in.at[j], mine_send.at[j], mine_recv.at[j],
            device_id={"seq": partner},
        )

    def far_copy(j):
        return pltpu.make_async_remote_copy(
            far_out.at[j], far_in.at[j], far_send.at[j], far_recv.at[j],
            device_id={"seq": across},
        )

    held = [None] * chunks

    def forward(j):
        near_copy(j).wait()
        far_out[j] = (held[j] + near_in[j].astype(F32)).astype(BF16)
        far_copy(j).start()

    for j in range(chunks):
        w = ow[:, j * chunk : (j + 1) * chunk]
        near_out[j] = jnp.dot(
            block((1 - half) * 2 + (1 - core)), w, preferred_element_type=F32
        ).astype(BF16)
        near_copy(j).start()
        held[j] = jnp.dot(block(across), w, preferred_element_type=F32)
        if j > 0:
            forward(j - 1)
    forward(chunks - 1)
    pass_on(wides - 1)
    for j in range(chunks):
        w = ow[:, j * chunk : (j + 1) * chunk]
        mine_out[j] = jnp.dot(block(partner), w, preferred_element_type=F32).astype(BF16)
        mine_copy(j).start()
        own[:, j * chunk : (j + 1) * chunk] = jnp.dot(
            block(seat), w, preferred_element_type=F32
        )
    for stage in range(q_stages):
        for kind in range(3):
            ctx_copy(stage, kind).wait()
    for i in range(wides):
        wide_copy(0, i).wait()
        wide_copy(2, i).wait()
        total = jnp.zeros((part, chunk), F32)
        for index in range(seq_count):
            total = total + jnp.dot(
                ctx_all[index], wide[index, i], preferred_element_type=F32
            )
        mixed_ref[:, i * chunk : (i + 1) * chunk] = total.astype(BF16)
    for j in range(chunks):
        mine_copy(j).wait()
        cols = slice(j * chunk, (j + 1) * chunk)
        own[:, cols] += mine_in[j].astype(F32)
    for j in range(chunks):
        far_copy(j).wait()
        cols = slice(j * chunk, (j + 1) * chunk)
        mixed_ref[:, (wides + j) * chunk : (wides + j + 1) * chunk] = (
            own[:, cols] + far_in[j].astype(F32)
        ).astype(BF16)


def per_device(
    tokens, positions, loss_mask, sample_tokens, dest_slot, norm_gain,
    q_weight, k_weight, v_weight, q_bias, k_bias, v_bias, o_weight,
):
    peers = lax.axis_size("dp")
    seq_count = lax.axis_size("seq")
    rows, depth = tokens.shape
    slot_count = 2 * BUCKET
    room = -(-(slot_count // peers) // 16) * 16
    group = math.gcd(peers, 8)
    q_heads = q_weight.shape[1] // DH
    kv_heads = k_weight.shape[1] // DH
    per_stage = math.gcd(q_heads, 2)
    stages = q_heads // per_stage
    strips = math.gcd(rows // 16, 4)
    part = slot_count // seq_count
    out_width = o_weight.shape[1]
    chunk = math.gcd(out_width, 512)
    wides = max(1, 3 * (out_width // chunk) // 7)
    chunks = out_width // chunk - wides
    kv_width = 2 * kv_heads * DH
    q_width = per_stage * DH
    vmem = pl.BlockSpec(memory_space=pltpu.VMEM)
    hbm = pl.BlockSpec(memory_space=pl.ANY)
    piece = pltpu.VMEM((chunks, part, chunk), BF16)
    dma = pltpu.SemaphoreType.DMA
    mixed, weight = pl.pallas_call(
        functools.partial(
            layer_kernel, peers, group, seq_count, q_heads, kv_heads, chunk, room, strips
        ),
        in_specs=[
            hbm, vmem, hbm, hbm, hbm, vmem, vmem, vmem, vmem, vmem, vmem, hbm,
        ],
        out_specs=[vmem, vmem],
        out_shape=[
            jax.ShapeDtypeStruct((part, out_width), BF16),
            jax.ShapeDtypeStruct((1, part), F32),
        ],
        scratch_shapes=[
            pltpu.VMEM((rows, depth), BF16),
            pltpu.VMEM((rows, 1), F32),
            pltpu.VMEM(q_weight.shape, BF16),
            pltpu.VMEM((depth, kv_width), BF16),
            pltpu.VMEM((o_weight.shape[0], chunks * chunk), BF16),
            pltpu.VMEM((peers * LANES, rows), BF16),
            pltpu.VMEM((peers, 8, LANES), F32),
            pltpu.VMEM((peers, 8, LANES), F32),
            pltpu.VMEM((stages, peers, room, q_width), BF16),
            pltpu.VMEM((stages, peers, room, q_width), BF16),
            pltpu.VMEM((peers, room, kv_width), BF16),
            pltpu.VMEM((peers, room, kv_width), BF16),
            pltpu.VMEM((slot_count, peers * LANES), BF16),
            pltpu.VMEM((peers * LANES, max(kv_width, q_width)), BF16),
            pltpu.VMEM((slot_count, q_heads * DH), BF16),
            pltpu.VMEM((slot_count, kv_width), BF16),
            pltpu.VMEM((slot_count, q_heads * DH), BF16),
            pltpu.VMEM((part, chunks * chunk), F32),
            piece, piece, piece, piece, piece, piece,
            pltpu.VMEM((rows, DH), F32),
            pltpu.VMEM((rows, DH), F32),
            pltpu.VMEM((seq_count, wides, o_weight.shape[0], chunk), BF16),
            pltpu.VMEM((seq_count, part, q_heads * DH), BF16),
            dma((stages + 1, peers)), dma((stages + 1, peers)), dma((peers,)), dma((peers,)),
            dma((chunks,)), dma((chunks,)), dma((chunks,)),
            dma((chunks,)), dma((chunks,)), dma((chunks,)),
            dma((strips + 4,)), dma((wides,)), dma((3, wides)), dma((3, wides)),
            dma((stages, 3)), dma((stages, 3)),
        ],
        compiler_params=pltpu.CompilerParams(
            collective_id=0, has_side_effects=True, vmem_limit_bytes=67043328
        ),
    )(
        tokens, norm_gain, q_weight, k_weight, v_weight, q_bias, k_bias, v_bias, positions,
        dest_slot, loss_mask, o_weight,
    )
    return (mixed, weight.reshape(part))


def solution(mesh):
    return jax.shard_map(
        per_device,
        mesh=mesh,
        in_specs=(
            P("dp", None),
            P(None, "dp"),
            P("dp"),
            P(),
            P("dp"),
            P(),
            P(None, "seq"),
            P(None, "seq"),
            P(None, "seq"),
            P("seq"),
            P("seq"),
            P("seq"),
            P("seq", None),
        ),
        out_specs=(P(("dp", "seq"), None), P(("dp", "seq"))),
        check_vma=False,
    )
```
